32 devices in a mesh: right: 4 (over z), left: 8 (over y, x, core).
Axes of the slice: x: 2, y: 2, z: 4, core: 2. Of those that a mesh axis runs over, the one named last changes fastest.
Arguments:
- psi_init: float32 [4096, 2, 2, 1024], P('left', None, None, 'right')
- left_env: float32 [4096, 5, 4096], P('left')
- right_env: float32 [1024, 5, 1024], P('right')
- mpo_two: float32 [5, 5, 2, 2, 2, 2], replicated
Outputs:
- output 1: float32 [4], replicated
- output 2: float32 [4], replicated
- output 3: float32 [4096, 2, 2, 1024], P('left', None, None, 'right')
All inputs are finite; a program needn't handle non-finite values.
Results may differ from the reference program's by a relative error of at most 0.001.
Values sent between devices are 32-bit elements.
A program may use at most 1 GiB of HBM per device.

```python
import jax
import jax.numpy as jnp
from jax import lax

PHYS_DIM = 2
MPO_DIM = 5
LEFT_BOND = 4096
RIGHT_BOND = 1024
LANCZOS_STEPS = 4
ROW_BLOCK = min(LEFT_BOND, 512)
ROW_COUNT = LEFT_BOND // ROW_BLOCK
PREC_HIGH = lax.Precision.HIGHEST


def sym_env(key_main, key_diag, bond_size):
    rand_part = jax.random.normal(key_main, (bond_size, MPO_DIM, bond_size), jnp.float32)
    shifts = jax.random.uniform(key_diag, (MPO_DIM,), jnp.float32, 0.5, 1.5)
    eye_mat = jnp.eye(bond_size, dtype=jnp.float32)
    sym_part = (rand_part + jnp.transpose(rand_part, (2, 1, 0))) * (2.0 * bond_size) ** -0.5
    return sym_part + shifts[None, :, None] * eye_mat[:, None, :]


def draw_mpo(key_main, key_diag):
    shape_six = (MPO_DIM, MPO_DIM, PHYS_DIM, PHYS_DIM, PHYS_DIM, PHYS_DIM)
    rand_part = jax.random.normal(key_main, shape_six, jnp.float32)
    sym_part = (rand_part + jnp.transpose(rand_part, (0, 1, 4, 5, 2, 3))) * (2.0 * MPO_DIM * MPO_DIM * PHYS_DIM * PHYS_DIM) ** -0.5
    weights = jax.random.uniform(key_diag, (MPO_DIM, MPO_DIM), jnp.float32, 0.5, 1.5) / (MPO_DIM * MPO_DIM)
    eye_phys = jnp.eye(PHYS_DIM * PHYS_DIM, dtype=jnp.float32).reshape(PHYS_DIM, PHYS_DIM, PHYS_DIM, PHYS_DIM)
    return sym_part + weights[:, :, None, None, None, None] * eye_phys[None, None]


def setup_inputs(seed: int = 0) -> dict:
    key_list = jax.random.split(jax.random.key(seed), 7)
    psi_init = jax.random.normal(key_list[0], (LEFT_BOND, PHYS_DIM, PHYS_DIM, RIGHT_BOND), jnp.float32)
    left_env = sym_env(key_list[1], key_list[2], LEFT_BOND)
    right_env = sym_env(key_list[3], key_list[4], RIGHT_BOND)
    mpo_two = draw_mpo(key_list[5], key_list[6])
    return {'psi_init': psi_init, 'left_env': left_env, 'right_env': right_env, 'mpo_two': mpo_two}


def apply_ham(vec_in, left_env, right_env, mpo_two):
    def one_block(block_idx):
        env_block = lax.dynamic_slice_in_dim(left_env, block_idx * ROW_BLOCK, ROW_BLOCK, axis=2)
        t_one = jnp.einsum('alc,astb->lcstb', env_block, vec_in, precision=PREC_HIGH)
        t_two = jnp.einsum('lcstb,lrstuv->cbruv', t_one, mpo_two, precision=PREC_HIGH)
        return jnp.einsum('cbruv,brd->cuvd', t_two, right_env, precision=PREC_HIGH)
    out_blocks = lax.map(one_block, jnp.arange(ROW_COUNT))
    return out_blocks.reshape(LEFT_BOND, PHYS_DIM, PHYS_DIM, RIGHT_BOND)


def reference(psi_init, left_env, right_env, mpo_two):
    elem_count = LEFT_BOND * PHYS_DIM * PHYS_DIM * RIGHT_BOND
    start_vec = psi_init * jnp.sqrt(elem_count / jnp.sum(psi_init * psi_init))

    def lanczos_step(step_carry, unused):
        vec_prev, vec_cur, beta_prev = step_carry
        next_vec = apply_ham(vec_cur, left_env, right_env, mpo_two)
        alpha_val = jnp.sum(vec_cur * next_vec) / elem_count
        next_vec = next_vec - alpha_val * vec_cur - beta_prev * vec_prev
        beta_val = jnp.sqrt(jnp.sum(next_vec * next_vec) / elem_count)
        return (vec_cur, next_vec / beta_val, beta_val), (alpha_val, beta_val)

    start_carry = (jnp.zeros_like(start_vec), start_vec, jnp.zeros((), jnp.float32))
    end_carry, step_outs = lax.scan(lanczos_step, start_carry, None, length=LANCZOS_STEPS)
    return step_outs[0], step_outs[1], end_carry[1]
```

```python
import functools

import jax
import jax.numpy as jnp
from jax import lax
from jax.experimental import pallas as pl
from jax.experimental.pallas import tpu as pltpu
from jax.sharding import PartitionSpec as P

LANCZOS_STEPS = 4
PREC = lax.Precision.HIGHEST
MESH = pl.DeviceIdType.MESH
F32 = jnp.float32

Z = 4
LEFT = 8
A = 512
B = 256
PH = 4
W = 5
C = 4
AL = A // C
S = C * PH
ROWS = PH * B


def scale_kernel(first, *refs):
    if first:
        coef_ref, g_ref, rt_ref, wb_ref, vn_ref, x_ref, vs_ref, u_ref = refs
    else:
        coef_ref, prev_ref, g_ref, vc_ref, vp_ref, rt_ref, wb_ref, vn_ref, x_ref, vs_ref, u_ref = refs
    inv = coef_ref[2:3, :]
    if not first:
        alpha = coef_ref[0:1, :]
        beta_prev = prev_ref[1:2, :]
    for z in range(Z):
        for st in range(PH):
            vec = g_ref[z, 0, st]
            if not first:
                vec = vec - alpha * vc_ref[z, 0, st] - beta_prev * vp_ref[z, 0, st]
            vec = vec * inv
            vn_ref[z, 0, st] = vec
            vs_ref[pl.ds(z * B, B), pl.ds(st * AL, AL)] = vec

    def right_dot(r, _):
        rows = pl.ds(pl.multiple_of(r * B, B), B)
        u_ref[r] = jnp.dot(rt_ref[rows, :], vs_ref[...], precision=PREC, preferred_element_type=F32)
        return 0

    lax.fori_loop(0, W, right_dot, 0)

    def mix(g, _):
        rows = pl.ds(pl.multiple_of(g * 8, 8), 8)
        parts = [u_ref[r, rows, pl.ds(st * AL, AL)] for r in range(W) for st in range(PH)]
        for l in range(W):
            for uv in range(PH):
                acc = None
                for i, part in enumerate(parts):
                    term = wb_ref[(l * PH + uv) * W * PH + i] * part
                    acc = term if acc is None else acc + term
                x_ref[l, pl.ds(pl.multiple_of(uv * B + g * 8, 8), 8), :] = acc
        return 0

    lax.fori_loop(0, B // 8, mix, 0)


def make_scale(first):
    tile = pl.BlockSpec((8, 128), lambda c: (0, 0))
    vec = pl.BlockSpec((Z, 1, PH, B, AL), lambda c: (0, c, 0, 0, 0))
    specs = [tile, vec] if first else [tile, tile, vec, vec, vec]
    specs += [
        pl.BlockSpec((W * B, Z * B), lambda c: (0, 0)),
        pl.BlockSpec((W * PH * W * PH, 8, 128), lambda c: (0, 0, 0)),
    ]
    return pl.pallas_call(
        functools.partial(scale_kernel, first),
        grid=(C,),
        in_specs=specs,
        out_specs=[vec, pl.BlockSpec((W, ROWS, AL), lambda c: (0, 0, c))],
        out_shape=[
            jax.ShapeDtypeStruct((Z, C, PH, B, AL), F32),
            jax.ShapeDtypeStruct((W, ROWS, A), F32),
        ],
        scratch_shapes=[pltpu.VMEM((Z * B, PH * AL), F32), pltpu.VMEM((W, B, PH * AL), F32)],
        compiler_params=pltpu.CompilerParams(vmem_limit_bytes=62 * 2**20),
        cost_estimate=pl.CostEstimate(flops=12 * W * B * Z * B * PH * A, bytes_accessed=60 * 2**20, transcendentals=0),
        name="scale_first" if first else "scale",
    )


def place(left):
    return left // 4, (left // 2) % 2, left % 2


def left_of(y, x, core):
    return (y * 2 + x) * 2 + core


def product_kernel(
    last, xs_hbm, lr_hbm, vc_hbm, vp_hbm, prev_ref, *refs
):
    if last:
        out_hbm, coef_ref = refs[:2]
    else:
        g_hbm, coef_ref = refs[:2]
    (xs, lb, pb, ra, sb, rb, w, v, vp, acc, ar_s, ar_r,
     x_sem, l_sem, v_sem, a_send, a_recv, b_send, b_recv, z_send, z_recv, r_send, r_recv, o_sem) = refs[2:]
    zi = lax.axis_index("right")
    li = lax.axis_index("left")
    y, x, core = place(li)
    peers = [
        (zi, left_of(y, x, 1 - core)),
        (zi, left_of(y, 1 - x, core)),
        (zi, left_of(1 - y, x, core)),
        (zi, left_of(1 - y, 1 - x, core)),
    ]
    z_near = (zi // 2) * 2 + 1 - zi % 2
    z_far = (zi + 2) % 4
    owner = [left_of(y, x, core), left_of(y, 1 - x, core), left_of(1 - y, x, core), left_of(1 - y, 1 - x, core),
             left_of(y, x, 1 - core), left_of(y, 1 - x, 1 - core), left_of(1 - y, x, 1 - core), left_of(1 - y, 1 - x, 1 - core)]

    def load_l(c, slot):
        for q in range(8):
            pltpu.make_async_copy(
                lr_hbm.at[c, :, :, pl.ds(pl.multiple_of(owner[q] * AL, AL), AL)],
                lb.at[slot, :, :, pl.ds(q * AL, AL)],
                l_sem.at[slot],
            ).start()

    x_copy = pltpu.make_async_copy(xs_hbm, xs, x_sem)
    x_copy.start()
    load_l(0, 0)
    v_copy = pltpu.make_async_copy(vc_hbm.at[zi], v, v_sem.at[0])
    v_copy.start()
    vp_copy = pltpu.make_async_copy(vp_hbm.at[zi], vp, v_sem.at[1])
    vp_copy.start()

    barrier = pltpu.get_barrier_semaphore()
    for peer in peers:
        pl.semaphore_signal(barrier, inc=1, device_id=peer, device_id_type=MESH)
    pl.semaphore_signal(barrier, inc=1, device_id=(z_far, li), device_id_type=MESH)
    if last:
        pl.semaphore_signal(barrier, inc=1, device_id=(z_near, li), device_id_type=MESH)
        pl.semaphore_wait(barrier, 6)
    else:
        @pl.when(zi > 0)
        def _():
            pl.semaphore_signal(barrier, inc=1, device_id=(zi - 1, li), device_id_type=MESH)

        @pl.when(zi < Z - 1)
        def _():
            pl.semaphore_signal(barrier, inc=1, device_id=(zi + 1, li), device_id_type=MESH)

        pl.semaphore_wait(barrier, 6 + ((zi + 1) // 2) % 2)

    acc[...] = jnp.zeros_like(acc)
    x_copy.wait()
    v_copy.wait()
    vp_copy.wait()

    def compute(i):
        c, u = i // PH, i % PH
        slot = c % 2

        @pl.when(u == 0)
        def _():
            pltpu.make_async_copy(lr_hbm.at[0], lb.at[slot], l_sem.at[slot]).wait()

            @pl.when(c < C - 1)
            def _():
                load_l(c + 1, 1 - slot)

        rows = pl.ds(pl.multiple_of(u * B, B), B)
        for half in range(2):
            tot = None
            for l in range(W):
                term = jnp.dot(
                    xs[l, rows, :], lb[slot, l, :, pl.ds(half * 4 * AL, 4 * AL)], precision=PREC, preferred_element_type=F32
                )
                tot = term if tot is None else tot + term
            for q in range(4):
                pb[i % 2, half * 4 + q] = tot[:, q * AL : (q + 1) * AL]

    def a_copy(i):
        return pltpu.make_async_remote_copy(
            src_ref=pb.at[i % 2, pl.ds(4, 4)], dst_ref=ra.at[i % 2], send_sem=a_send.at[i % 2], recv_sem=a_recv.at[i % 2],
            device_id=peers[0], device_id_type=MESH)

    def b_copy(i, k):
        return pltpu.make_async_remote_copy(
            src_ref=sb.at[i % 2, k + 1], dst_ref=rb.at[i % 2, k], send_sem=b_send.at[i % 2, k], recv_sem=b_recv.at[i % 2, k],
            device_id=peers[k + 1], device_id_type=MESH)

    def stage_b(i):
        a_copy(i).wait()
        for q in range(4):
            sb[i % 2, q] = pb[i % 2, q] + ra[i % 2, q]
        for k in (2, 0, 1):
            b_copy(i, k).start()

    def z_copy(up, hop, i):
        src_z = zi - (hop - 1) if up else zi + (hop - 1)
        src = w.at[i // PH, i % PH] if hop == 1 else g_hbm.at[src_z, i // PH, i % PH]
        return pltpu.make_async_remote_copy(
            src_ref=src, dst_ref=g_hbm.at[src_z, i // PH, i % PH],
            send_sem=z_send.at[0 if up else 1, hop - 1, i], recv_sem=z_recv.at[0 if up else 1, hop - 1, i],
            device_id=(zi + 1 if up else zi - 1, li), device_id_type=MESH)

    def z_sends(hop, up):
        return (zi < Z - 1) & (zi >= hop - 1) if up else (zi > 0) & (zi + hop - 1 <= Z - 1)

    def z_gets(hop, up):
        return zi >= hop if up else zi + hop <= Z - 1

    def z_start(hop, i):
        for up in (True, False):
            @pl.when(z_sends(hop, up))
            def _(up=up):
                z_copy(up, hop, i).start()

    def z_landed(up, hop, i):
        src_z = zi - hop if up else zi + hop
        ref = g_hbm.at[src_z, i // PH, i % PH]
        return pltpu.make_async_remote_copy(
            src_ref=ref, dst_ref=ref,
            send_sem=z_send.at[0 if up else 1, hop - 1, i], recv_sem=z_recv.at[0 if up else 1, hop - 1, i],
            device_id=(zi - 1 if up else zi + 1, li), device_id_type=MESH)

    def stage_h(hop, i):
        for up in (True, False):
            @pl.when(z_gets(hop, up))
            def _(up=up):
                z_landed(up, hop, i).wait_recv()
        if hop < 3:
            z_start(hop + 1, i)

    def own_copy(i):
        return pltpu.make_async_copy(w.at[i // PH, i % PH], g_hbm.at[zi, i // PH, i % PH], o_sem.at[i])

    def stage_c(i):
        for k in range(3):
            b_copy(i, k).wait()
        c, u = i // PH, i % PH
        val = (sb[i % 2, 0] + rb[i % 2, 2]) + (rb[i % 2, 0] + rb[i % 2, 1])
        w[c, u] = val
        prod = (val * v[c, u]).reshape(B // 8, 8, AL)
        acc[0] += jnp.sum(prod, axis=0)
        if not last:
            z_start(1, i)
            own_copy(i).start()

    def boundary(i, _):
        @pl.when(i < S)
        def _():
            compute(i)

        @pl.when((i >= 2))
        def _():
            stage_c(i - 2)

        if not last:
            @pl.when((i >= 4))
            def _():
                stage_h(1, i - 4)

            @pl.when((i >= 6))
            def _():
                stage_h(2, i - 6)

            @pl.when((i >= 8))
            def _():
                stage_h(3, i - 8)

        @pl.when((i >= 1) & (i < S + 1))
        def _():
            stage_b(i - 1)

        @pl.when(i < S)
        def _():
            a_copy(i).start()

        return 0

    lax.fori_loop(0, S + 2, boundary, 0)

    def drain(hop, i):
        if not last:
            stage_h(hop, i)

    ring = [peers[0], peers[1], peers[2], (z_near, li), (z_far, li)]

    def reduce_round(ph, r):
        copy = pltpu.make_async_remote_copy(
            src_ref=ar_s.at[ph, r], dst_ref=ar_r.at[ph, r], send_sem=r_send.at[ph, r], recv_sem=r_recv.at[ph, r],
            device_id=ring[r], device_id_type=MESH)
        ar_s[ph, r] = acc[ph]
        copy.start()
        copy.wait()
        acc[ph] = ar_s[ph, r] + ar_r[ph, r]

    count = float(LEFT * Z * S * B * AL)
    reduce_round(0, 0)
    drain(1, S - 2)
    drain(2, S - 4)
    reduce_round(0, 1)
    reduce_round(0, 2)
    drain(1, S - 1)
    drain(2, S - 3)
    reduce_round(0, 3)
    reduce_round(0, 4)
    alpha = jnp.sum(acc[0]) / count
    beta_prev = prev_ref[1:2, :]

    def ortho(i, _):
        c, u = i // PH, i % PH
        val = w[c, u] - alpha * v[c, u] - beta_prev * vp[c, u]
        if last:
            w[c, u] = val
        acc[1] += jnp.sum((val * val).reshape(B // 8, 8, AL), axis=0)
        return 0

    lax.fori_loop(0, S, ortho, 0)
    reduce_round(1, 0)
    drain(2, S - 2)
    reduce_round(1, 1)
    drain(2, S - 1)
    reduce_round(1, 2)
    reduce_round(1, 3)
    reduce_round(1, 4)
    beta = jnp.sqrt(jnp.full((1, 128), jnp.sum(acc[1]) / count, F32))
    inv = 1.0 / beta
    coef_ref[0:1, :] = jnp.full((1, 128), alpha, F32)
    coef_ref[1:2, :] = beta
    coef_ref[2:3, :] = inv
    coef_ref[3:8, :] = jnp.zeros((5, 128), F32)
    if last:
        def final(i, _):
            w[i // PH, i % PH] = w[i // PH, i % PH] * inv
            return 0

        lax.fori_loop(0, S, final, 0)
        copy = pltpu.make_async_copy(w, out_hbm, o_sem.at[0])
        copy.start()
        copy.wait()
    else:
        def finish(i, _):
            @pl.when(i >= S - 6)
            def _():
                stage_h(3, i)

            own_copy(i).wait()
            for hop in (1, 2, 3):
                for up in (True, False):
                    @pl.when(z_sends(hop, up))
                    def _(up=up, hop=hop):
                        z_copy(up, hop, i).wait_send()
            return 0

        lax.fori_loop(0, S, finish, 0)


def make_product(last):
    hbm = pl.BlockSpec(memory_space=pltpu.HBM)
    vmem = pl.BlockSpec(memory_space=pltpu.VMEM)
    dma = pltpu.SemaphoreType.DMA
    big = (C, PH, B, AL) if last else (Z, C, PH, B, AL)
    piece = (B, AL)
    return pl.pallas_call(
        functools.partial(product_kernel, last),
        in_specs=[hbm, hbm, hbm, hbm, vmem],
        out_specs=[hbm, vmem],
        out_shape=[jax.ShapeDtypeStruct(big, F32), jax.ShapeDtypeStruct((8, 128), F32)],
        scratch_shapes=[
            pltpu.VMEM((W, ROWS, A), F32),
            pltpu.VMEM((2, W, A, LEFT * AL), F32),
            pltpu.VMEM((2, 8) + piece, F32),
            pltpu.VMEM((2, 4) + piece, F32),
            pltpu.VMEM((2, 4) + piece, F32),
            pltpu.VMEM((2, 3) + piece, F32),
            pltpu.VMEM((C, PH) + piece, F32),
            pltpu.VMEM((C, PH) + piece, F32),
            pltpu.VMEM((C, PH) + piece, F32),
            pltpu.VMEM((2, 8, 128), F32),
            pltpu.VMEM((2, 5, 8, 128), F32),
            pltpu.VMEM((2, 5, 8, 128), F32),
            dma, dma((2,)), dma((2,)), dma((2,)), dma((2,)), dma((2, 3)), dma((2, 3)),
            dma((2, 3, S)), dma((2, 3, S)), dma((2, 5)), dma((2, 5)), dma((S,)),
        ],
        compiler_params=pltpu.CompilerParams(
            vmem_limit_bytes=62 * 2**20, collective_id=2 if last else 1, has_side_effects=True),
        cost_estimate=pl.CostEstimate(flops=12 * W * A * ROWS * LEFT * A, bytes_accessed=60 * 2**20, transcendentals=0),
        name="product_last" if last else "product",
    )


def solution(mesh):
    count = float(mesh.shape["left"] * mesh.shape["right"])

    def lanczos(psi, left_env, right_env, mpo):
        left_idx = lax.axis_index("left")
        total = lax.psum(jnp.sum(psi * psi), ("left", "right"))
        own = psi.reshape(C, AL, PH, B).transpose(0, 2, 3, 1)
        gathered = lax.all_gather(own, "right", axis=0)
        l_env = left_env.reshape(A, W, LEFT, C, AL).transpose(3, 1, 0, 2, 4).reshape(C, W, A, LEFT * AL)
        part = lax.dynamic_slice_in_dim(right_env, left_idx * (B // LEFT), B // LEFT, axis=0)
        part = lax.all_to_all(part, "right", split_axis=2, concat_axis=0, tiled=True)
        part = part.reshape(Z, B // LEFT, W, B).transpose(2, 3, 0, 1)
        r_env = lax.all_gather(part, "left", axis=0)
        r_env = r_env.transpose(1, 2, 3, 0, 4).reshape(W * B, Z * B)
        mix = mpo.reshape(W, W, PH, PH).transpose(0, 3, 1, 2).reshape(-1, 1, 1)
        mix = jnp.broadcast_to(mix, (W * PH * W * PH, 8, 128))
        scale0 = jnp.sqrt(psi.size * count / total)
        coef = jnp.zeros((8, 128), F32).at[2, :].set(scale0)
        prev = jnp.zeros((8, 128), F32)
        first, scale = make_scale(True), make_scale(False)
        product, product_last = make_product(False), make_product(True)
        coefs = []
        v_cur, x_env = first(coef, gathered, r_env, mix)
        v_prev = v_cur
        for j in range(LANCZOS_STEPS):
            if j < LANCZOS_STEPS - 1:
                g, coef = product(x_env, l_env, v_cur, v_prev, prev)
            else:
                out, coef = product_last(x_env, l_env, v_cur, v_prev, prev)
            coefs.append(coef)
            if j < LANCZOS_STEPS - 1:
                v_next, x_env = scale(coef, prev, g, v_cur, v_prev, r_env, mix)
                v_prev, v_cur = v_cur, v_next
            prev = coef
        alpha = jnp.stack([c[0, 0] for c in coefs])
        beta = jnp.stack([c[1, 0] for c in coefs])
        vec = out.transpose(0, 3, 1, 2).reshape(psi.shape)
        return alpha, beta, vec

    return jax.shard_map(
        lanczos,
        mesh=mesh,
        in_specs=(P("left", None, None, "right"), P("left", None, None), P("right", None, None), P()),
        out_specs=(P(), P(), P("left", None, None, "right")),
        check_vma=False,
    )
```

```python
import functools

import jax
import jax.numpy as jnp
from jax import lax
from jax.experimental import pallas as pl
from jax.experimental.pallas import tpu as pltpu
from jax.sharding import PartitionSpec as P

STEPS = 4
PREC = lax.Precision.HIGHEST
MESH = pl.DeviceIdType.MESH
F32 = jnp.float32

Z = 4
LEFT = 8
A = 512
B = 256
PH = 4
W = 5
C = 4
AL = A // C
S = C * PH
Q = 4
D = B // Q
SUB = B // LEFT
COUNT = float(LEFT * Z * S * B * AL)


def place(left):
    return left // 4, (left // 2) % 2, left % 2


def left_of(y, x, core):
    return (y * 2 + x) * 2 + core


def rows8(value):
    return jnp.sum(value.reshape(-1, 8, AL), axis=0)


def kernel(psi_hbm, l_hbm, r_hbm, wb, out_hbm, coef_ref, hist_hbm,
           xs, lb, pb, ra, sb, rb, gb, vv, rt, us, xb, cf, acc, ar_s, ar_r,
           p_sem, l_sem, h_sem, x_sem, o_sem, r1_send, r1_recv, r2_send, r2_recv, r_own,
           a_send, a_recv, b_send, b_recv, z_send, z_recv, ar_send, ar_recv, ready):
    zi = lax.axis_index("right")
    li = lax.axis_index("left")
    y, x, core = place(li)
    owner = [left_of(y, x, core), left_of(y, 1 - x, core), left_of(1 - y, x, core), left_of(1 - y, 1 - x, core),
             left_of(y, x, 1 - core), left_of(y, 1 - x, 1 - core), left_of(1 - y, x, 1 - core), left_of(1 - y, 1 - x, 1 - core)]
    z_near = (zi // 2) * 2 + 1 - zi % 2
    z_far = (zi + 2) % 4
    ring = [(zi, owner[4]), (zi, owner[1]), (zi, owner[2]), (z_near, li), (z_far, li)]

    def load_l(c, slot):
        for q in range(LEFT):
            pltpu.make_async_copy(
                l_hbm.at[:, :, pl.ds(pl.multiple_of(owner[q] * A + c * AL, AL), AL)],
                lb.at[slot, :, :, pl.ds(q * AL, AL)],
                l_sem.at[slot],
            ).start()

    def wait_l(slot):
        pltpu.make_async_copy(l_hbm.at[:, :, pl.ds(0, LEFT * AL)], lb.at[slot], l_sem.at[slot]).wait()

    psi_copy = pltpu.make_async_copy(psi_hbm, vv.at[0], p_sem)
    psi_copy.start()

    barrier = pltpu.get_barrier_semaphore()
    for q in range(1, LEFT):
        pl.semaphore_signal(barrier, inc=1, device_id=(zi, owner[q]), device_id_type=MESH)
    for k in range(1, Z):
        pl.semaphore_signal(barrier, inc=1, device_id=((zi + k) % Z, li), device_id_type=MESH)
    pl.semaphore_wait(barrier, LEFT + Z - 2)

    def rt_rows(left):
        return left // 2, pl.ds(pl.multiple_of((left % 2) * SUB, SUB), SUB)

    my_q, my_rows = rt_rows(li)

    def r_first(k):
        dest = (zi + k) % Z
        return pltpu.make_async_remote_copy(
            src_ref=r_hbm.at[:, pl.ds(pl.multiple_of(dest * B + li * SUB, SUB), SUB), :],
            dst_ref=rt.at[my_q, :, my_rows, pl.ds(pl.multiple_of(zi * B, B), B)],
            send_sem=r1_send.at[k - 1], recv_sem=r1_recv.at[k - 1], device_id=(dest, li), device_id_type=MESH)

    def r_second(q):
        ref = rt.at[my_q, :, my_rows, :]
        return pltpu.make_async_remote_copy(
            src_ref=ref, dst_ref=ref, send_sem=r2_send.at[q - 1], recv_sem=r2_recv.at[q - 1],
            device_id=(zi, owner[q]), device_id_type=MESH)

    def r_second_landed(q):
        peer_q, peer_rows = rt_rows(owner[q])
        ref = rt.at[peer_q, :, peer_rows, :]
        return pltpu.make_async_remote_copy(
            src_ref=ref, dst_ref=ref, send_sem=r2_send.at[q - 1], recv_sem=r2_recv.at[q - 1],
            device_id=(zi, owner[q]), device_id_type=MESH)

    for k in range(1, Z):
        r_first(k).start()
    r_mine = pltpu.make_async_copy(
        r_hbm.at[:, pl.ds(pl.multiple_of(zi * B + li * SUB, SUB), SUB), :],
        rt.at[my_q, :, my_rows, pl.ds(pl.multiple_of(zi * B, B), B)], r_own)
    r_mine.start()
    load_l(0, 0)

    def ar_copy(idx, r):
        return pltpu.make_async_remote_copy(
            src_ref=ar_s.at[idx, r], dst_ref=ar_r.at[idx, r], send_sem=ar_send.at[idx, r], recv_sem=ar_recv.at[idx, r],
            device_id=ring[r], device_id_type=MESH)

    def ar_start(idx, r):
        ar_s[idx, r] = acc[...]
        ar_copy(idx, r).start()

    def ar_finish(idx, r):
        ar_copy(idx, r).wait()
        acc[...] = ar_s[idx, r] + ar_r[idx, r]

    def gb_piece(src_z, i):
        return gb.at[i // PH, pl.ds(pl.multiple_of(src_z * B, B), B), pl.ds(pl.multiple_of((i % PH) * AL, AL), AL)]

    def z_copy(up, hop, i):
        src_z = zi - (hop - 1) if up else zi + (hop - 1)
        return pltpu.make_async_remote_copy(
            src_ref=gb_piece(src_z, i), dst_ref=gb_piece(src_z, i),
            send_sem=z_send.at[0 if up else 1, hop - 1, i], recv_sem=z_recv.at[0 if up else 1, hop - 1, i],
            device_id=(zi + 1 if up else zi - 1, li), device_id_type=MESH)

    def z_sends(hop, up):
        return (zi < Z - 1) & (zi >= hop - 1) if up else (zi > 0) & (zi + hop - 1 <= Z - 1)

    def z_start(hop, i):
        for up in (True, False):
            @pl.when(z_sends(hop, up))
            def _(up=up):
                z_copy(up, hop, i).start()

    def z_landed(up, hop, i):
        ref = gb_piece(zi - hop if up else zi + hop, i)
        return pltpu.make_async_remote_copy(
            src_ref=ref, dst_ref=ref,
            send_sem=z_send.at[0 if up else 1, hop - 1, i], recv_sem=z_recv.at[0 if up else 1, hop - 1, i],
            device_id=(zi - 1 if up else zi + 1, li), device_id_type=MESH)

    def stage_h(hop, i):
        for up in (True, False):
            @pl.when(zi >= hop if up else zi + hop <= Z - 1)
            def _(up=up):
                z_landed(up, hop, i).wait_recv()
        if hop < 3:
            z_start(hop + 1, i)

    def compute(s, i, part):
        c, u = i // PH, i % PH
        slot = c % 2

        @pl.when((u == 0) & (part == 0))
        def _():
            wait_l(slot)

            @pl.when((c < C - 1) | (s < STEPS))
            def _():
                load_l((c + 1) % C, 1 - slot)

        first = pl.multiple_of((1 - part) * 4 * AL, 4 * AL)
        tot = None
        for l in range(W):
            term = jnp.dot(
                xs[l, u].reshape(B, A), lb[slot, l, :, pl.ds(first, 4 * AL)], precision=PREC, preferred_element_type=F32
            )
            tot = term if tot is None else tot + term
        for q in range(4):
            pb[i % 2, (1 - part) * 4 + q] = tot[:, q * AL : (q + 1) * AL]

    def a_copy(i):
        return pltpu.make_async_remote_copy(
            src_ref=pb.at[i % 2, pl.ds(4, 4)], dst_ref=ra.at[i % 2], send_sem=a_send.at[i % 2], recv_sem=a_recv.at[i % 2],
            device_id=(zi, owner[4]), device_id_type=MESH)

    def b_copy(i, k):
        return pltpu.make_async_remote_copy(
            src_ref=sb.at[i % 2, k + 1], dst_ref=rb.at[i % 2, k], send_sem=b_send.at[i % 2, k], recv_sem=b_recv.at[i % 2, k],
            device_id=(zi, owner[k + 1]), device_id_type=MESH)

    def stage_b(i):
        a_copy(i).wait()
        for q in range(4):
            sb[i % 2, q] = pb[i % 2, q] + ra[i % 2, q]

    def stage_b_send(i):
        for k in (2, 0, 1):
            b_copy(i, k).start()

    def stage_c(s, i):
        for k in range(3):
            b_copy(i, k).wait()
        c, u = i // PH, i % PH
        val = (sb[i % 2, 0] + rb[i % 2, 2]) + (rb[i % 2, 0] + rb[i % 2, 1])
        gb[c, pl.ds(pl.multiple_of(zi * B, B), B), pl.ds(pl.multiple_of(u * AL, AL), AL)] = val
        acc[...] += rows8(val * vv[(s + 1) % 2, c, u])

    def right_dot(t, slot):
        us[slot] = jnp.dot(rt[t % Q].reshape(W * D, Z * B), gb[t // Q], precision=PREC, preferred_element_type=F32)

    def mix(t, slot):
        c, dq = t // Q, t % Q
        beta_prev = cf[1:2, :]
        for g in range(0, D // 8, 2):
            parts = [[us[slot, pl.ds(r * D + (g + k) * 8, 8), pl.ds(st * AL, AL)] for k in range(2)]
                     for r in range(W) for st in range(PH)]
            for l in range(W):
                for uv in range(PH):
                    tot = [None, None]
                    for j, part in enumerate(parts):
                        coef = wb[(l * PH + uv) * W * PH + j]
                        for k in range(2):
                            term = coef * part[k]
                            tot[k] = term if tot[k] is None else tot[k] + term
                    for k in range(2):
                        old = xb[slot, l, uv, pl.ds((g + k) * 8, 8), :]
                        row = pl.multiple_of((uv % 2) * B + dq * D + (g + k) * 8, 8)
                        lane = pl.multiple_of((uv // 2) * A + c * AL, AL)
                        lb[1, l, pl.ds(row, 8), pl.ds(lane, AL)] = tot[k] - beta_prev * old

    def old_copy(s, t, slot):
        return pltpu.make_async_copy(
            hist_hbm.at[s % 2, :, :, t % Q, :, pl.ds(pl.multiple_of((t // Q) * AL, AL), AL)], xb.at[slot], x_sem.at[slot])

    def hist_copy(s):
        return pltpu.make_async_copy(xs, hist_hbm.at[(s + 1) % 2], h_sem)

    def clear(i, _):
        for l in range(W):
            for h in range(4):
                xs[l, h, i] = jnp.zeros((D, A), F32)
        return 0

    lax.fori_loop(0, Q, clear, 0)
    us[...] = jnp.zeros_like(us)
    xb[...] = jnp.zeros_like(xb)
    vv[1] = jnp.zeros((C, PH, B, AL), F32)
    cf[...] = jnp.zeros_like(cf)
    cf[2:3, :] = jnp.ones((1, AL), F32)
    acc[...] = jnp.zeros_like(acc)
    psi_copy.wait()

    def norm(i, _):
        val = vv[0, i // PH, i % PH]
        acc[...] += rows8(val * val)
        return 0

    lax.fori_loop(0, S, norm, 0)
    for r in range(5):
        ar_start(0, r)
        ar_finish(0, r)
    scale = jnp.sqrt(COUNT / jnp.full((1, AL), jnp.sum(acc[...]), F32))

    def to_unit(i, _):
        c, u = i // PH, i % PH
        val = vv[0, c, u] * scale
        vv[0, c, u] = val
        gb[c, pl.ds(pl.multiple_of(zi * B, B), B), pl.ds(pl.multiple_of(u * AL, AL), AL)] = val
        return 0

    lax.fori_loop(0, S, to_unit, 0)

    def gather_step(i):
        @pl.when(i < S)
        def _():
            z_start(1, i)

        @pl.when((i >= 2) & (i < S + 2))
        def _():
            stage_h(1, i - 2)

        @pl.when((i >= 4) & (i < S + 4))
        def _():
            stage_h(2, i - 4)

    LEAD = 10

    def gather(i, _):
        gather_step(i)

        @pl.when(i == 3)
        def _():
            r_mine.wait()
            for k in range(1, Z):
                r_first(k).wait()
            for q in range(1, LEFT):
                r_second(q).start()

        return 0

    lax.fori_loop(0, LEAD, gather, 0)
    for q in range(1, LEFT):
        r_second(q).wait_send()
        r_second_landed(q).wait_recv()

    def step(s, _):
        @pl.when(s > 0)
        def _():
            acc[...] = jnp.zeros_like(acc)

            def half_step(h, _):
                i, part = h // 2, h % 2
                compute(s, i, part)

                @pl.when(part == 1)
                def _():
                    stage_b(i)

                    @pl.when(i >= 1)
                    def _():
                        stage_c(s, i - 1)

                    stage_b_send(i)

                    @pl.when(s < STEPS)
                    def _():
                        @pl.when(i == 1)
                        def _():
                            @pl.when(zi < Z - 1)
                            def _():
                                pl.semaphore_wait(ready.at[0], 1)

                            @pl.when(zi > 0)
                            def _():
                                pl.semaphore_wait(ready.at[1], 1)

                        @pl.when(i >= 3)
                        def _():
                            stage_h(2, i - 3)

                        @pl.when(i >= 2)
                        def _():
                            stage_h(1, i - 2)

                        @pl.when(i >= 1)
                        def _():
                            z_start(1, i - 1)

                @pl.when(part == 0)
                def _():
                    a_copy(i).start()

                return 0

            lax.fori_loop(0, 2 * S, half_step, 0)

        @pl.when((s > 0) & (s < STEPS))
        def _():
            hist_copy(s).start()

        def right_step(t, _):
            slot = t % 2

            @pl.when(s < STEPS)
            def _():
                @pl.when(t % Q == 0)
                def _():
                    for k in range(4):
                        stage_h(3, (t // Q) * 4 + k)

                @pl.when(s > 1)
                def _():
                    old_copy(s, t, slot).start()

                    @pl.when(t > 0)
                    def _():
                        old_copy(s, t - 1, 1 - slot).wait()

                right_dot(t, slot)
                mix(jnp.maximum(t - 1, 0), 1 - slot)

            @pl.when(s == 0)
            def _():
                gather_step(t + LEAD)

            @pl.when(s > 0)
            def _():
                idx = s * 2 - 1

                def at(when, fn, hop=False):
                    @pl.when((t == when) & (s < STEPS) if hop else t == when)
                    def _():
                        fn()

                at(1, lambda: (stage_h(2, S - 3), stage_h(1, S - 2)), True)
                at(3, lambda: stage_c(s, S - 1))
                at(3, lambda: ar_start(idx, 0))
                at(3, lambda: z_start(1, S - 1), True)
                at(4, lambda: stage_h(2, S - 2), True)
                for r in range(4):
                    at(4 + r, lambda r=r: (ar_finish(idx, r), ar_start(idx, r + 1)))
                at(5, lambda: stage_h(1, S - 1), True)
                at(7, lambda: stage_h(2, S - 1), True)

                def ortho():
                    ar_finish(idx, 4)
                    alpha = jnp.full((1, AL), jnp.sum(acc[...]) / COUNT, F32)
                    beta_prev = cf[1:2, :]
                    cf[0:1, :] = alpha
                    acc[...] = jnp.zeros_like(acc)

                    def piece(i, _):
                        c, u = i // PH, i % PH
                        val = gb[c, pl.ds(pl.multiple_of(zi * B, B), B), pl.ds(pl.multiple_of(u * AL, AL), AL)]
                        val = val - alpha * vv[(s + 1) % 2, c, u] - beta_prev * vv[s % 2, c, u]
                        vv[s % 2, c, u] = val
                        acc[...] += rows8(val * val)
                        return 0

                    lax.fori_loop(0, S, piece, 0)
                    ar_start(idx + 1, 0)

                at(8, ortho)
                for r in range(4):
                    at(9 + r, lambda r=r: (ar_finish(idx + 1, r), ar_start(idx + 1, r + 1)))

                def norm_out():
                    ar_finish(idx + 1, 4)
                    beta = jnp.sqrt(jnp.full((1, AL), jnp.sum(acc[...]) / COUNT, F32))
                    inv = 1.0 / beta
                    cf[2:3, :] = inv
                    cf[3:4, :] = beta
                    coef_ref[s - 1, 0:1, :] = cf[0:1, :]
                    coef_ref[s - 1, 1:2, :] = beta

                    def piece(i, _):
                        vv[s % 2, i // PH, i % PH] = vv[s % 2, i // PH, i % PH] * inv
                        return 0

                    lax.fori_loop(0, S, piece, 0)

                at(13, norm_out)

            return 0

        lax.fori_loop(0, S, right_step, 0)

        @pl.when(s < STEPS)
        def _():
            @pl.when(s > 1)
            def _():
                old_copy(s, S - 1, (S - 1) % 2).wait()

            mix(S - 1, (S - 1) % 2)

            @pl.when(s > 0)
            def _():
                hist_copy(s).wait()

            alpha, inv = cf[0:1, 0:1], cf[2:3, 0:1]

            def combine(k, _):
                l, uv = k // PH, k % PH
                for dq in range(Q):
                    new = lb[1, l, pl.ds(pl.multiple_of((uv % 2) * B + dq * D, D), D), pl.ds(pl.multiple_of((uv // 2) * A, A), A)]
                    xs[l, uv, dq] = (new - alpha * xs[l, uv, dq]) * inv
                return 0

            lax.fori_loop(0, W * PH, combine, 0)

            def sent(i, _):
                for hop in (1, 2, 3):
                    for up in (True, False):
                        @pl.when(z_sends(hop, up))
                        def _(up=up, hop=hop):
                            z_copy(up, hop, i).wait_send()
                return 0

            lax.fori_loop(0, S, sent, 0)

            @pl.when((zi > 0) & (s < STEPS - 1))
            def _():
                pl.semaphore_signal(ready.at[0], inc=1, device_id=(zi - 1, li), device_id_type=MESH)

            @pl.when((zi < Z - 1) & (s < STEPS - 1))
            def _():
                pl.semaphore_signal(ready.at[1], inc=1, device_id=(zi + 1, li), device_id_type=MESH)

            cf[1:2, :] = cf[3:4, :]

        return 0

    lax.fori_loop(0, STEPS + 1, step, 0)

    copy = pltpu.make_async_copy(vv.at[STEPS % 2], out_hbm, o_sem)
    copy.start()
    copy.wait()


def lanczos_kernel(psi, l_env, r_env, mix):
    hbm = pl.BlockSpec(memory_space=pltpu.HBM)
    vmem = pl.BlockSpec(memory_space=pltpu.VMEM)
    dma = pltpu.SemaphoreType.DMA
    piece = (B, AL)
    n_ar = 2 * STEPS + 1
    return pl.pallas_call(
        kernel,
        in_specs=[hbm, hbm, hbm, vmem],
        out_specs=[hbm, vmem, hbm],
        out_shape=[
            jax.ShapeDtypeStruct((C, PH) + piece, F32),
            jax.ShapeDtypeStruct((STEPS, 8, AL), F32),
            jax.ShapeDtypeStruct((2, W, PH, Q, D, A), F32),
        ],
        scratch_shapes=[
            pltpu.VMEM((W, PH, Q, D, A), F32),
            pltpu.VMEM((2, W, A, LEFT * AL), F32),
            pltpu.VMEM((2, 8) + piece, F32),
            pltpu.VMEM((2, 4) + piece, F32),
            pltpu.VMEM((2, 4) + piece, F32),
            pltpu.VMEM((2, 3) + piece, F32),
            pltpu.VMEM((C, Z * B, PH * AL), F32),
            pltpu.VMEM((2, C, PH) + piece, F32),
            pltpu.VMEM((Q, W, D, Z * B), F32),
            pltpu.VMEM((2, W * D, PH * AL), F32),
            pltpu.VMEM((2, W, PH, D, AL), F32),
            pltpu.VMEM((8, AL), F32),
            pltpu.VMEM((8, AL), F32),
            pltpu.VMEM((n_ar, 5, 8, AL), F32),
            pltpu.VMEM((n_ar, 5, 8, AL), F32),
            dma, dma((2,)), dma, dma((2,)), dma, dma((3,)), dma((3,)), dma((7,)), dma((7,)), dma,
            dma((2,)), dma((2,)), dma((2, 3)), dma((2, 3)), dma((2, 3, S)), dma((2, 3, S)),
            dma((n_ar, 5)), dma((n_ar, 5)), pltpu.SemaphoreType.REGULAR((2,)),
        ],
        compiler_params=pltpu.CompilerParams(
            vmem_limit_bytes=67_043_328, collective_id=1, has_side_effects=True),
        name="lanczos",
    )(psi, l_env, r_env, mix)


def solution(mesh):
    def lanczos(psi, left_env, right_env, mpo):
        own = psi.reshape(C, AL, PH, B).transpose(0, 2, 3, 1)
        l_env = left_env.transpose(1, 0, 2)
        r_env = right_env.transpose(1, 2, 0)
        mix = mpo.reshape(W, W, PH, PH).transpose(0, 3, 1, 2).reshape(-1, 1, 1)
        mix = jnp.broadcast_to(mix, (W * PH * W * PH, 8, AL))
        out, coef, _ = lanczos_kernel(own, l_env, r_env, mix)
        vec = out.transpose(0, 3, 1, 2).reshape(psi.shape)
        return coef[:, 0, 0], coef[:, 1, 0], vec

    return jax.shard_map(
        lanczos,
        mesh=mesh,
        in_specs=(P("left", None, None, "right"), P("left", None, None), P("right", None, None), P()),
        out_specs=(P(), P(), P("left", None, None, "right")),
        check_vma=False,
    )
```

```python
import jax
import jax.numpy as jnp
from jax import lax
from jax.experimental import pallas as pl
from jax.experimental.pallas import tpu as pltpu
from jax.sharding import PartitionSpec as P

STEPS = 4
PREC = lax.Precision.HIGHEST
MESH = pl.DeviceIdType.MESH
F32 = jnp.float32

Z = 4
LEFT = 8
A = 512
B = 256
PH = 4
W = 5
C = 4
AL = A // C
S = C * PH
Q = 2
D = B // Q
SUB = B // LEFT
RT = C * Q
COUNT = float(LEFT * Z * S * B * AL)


def place(left):
    return left // 4, (left // 2) % 2, left % 2


def left_of(y, x, core):
    return (y * 2 + x) * 2 + core


def rows8(value):
    return jnp.sum(value.reshape(-1, 8, AL), axis=0)


def kernel(psi_hbm, l_hbm, r_hbm, wb, out_hbm, coef_ref, hist_hbm,
           xs, lb, pb, ra, sb, rb, gb, vv, rt, us, xb, cf, acc, ar_p, ar_z,
           p_sem, l_sem, h_sem, x_sem, o_sem, r1_send, r1_recv, r2_send, r2_recv, r_own,
           a_send, a_recv, b_send, b_recv, z_send, z_recv, ar_send, ar_recv, ready):
    zi = lax.axis_index("right")
    li = lax.axis_index("left")
    y, x, core = place(li)
    owner = [left_of(y, x, core), left_of(y, 1 - x, core), left_of(1 - y, x, core), left_of(1 - y, 1 - x, core),
             left_of(y, x, 1 - core), left_of(y, 1 - x, 1 - core), left_of(1 - y, x, 1 - core), left_of(1 - y, 1 - x, 1 - core)]

    def load_l(c, slot):
        for q in range(LEFT):
            pltpu.make_async_copy(
                l_hbm.at[:, :, pl.ds(pl.multiple_of(owner[q] * A + c * AL, AL), AL)],
                lb.at[slot, :, :, pl.ds(q * AL, AL)],
                l_sem.at[slot],
            ).start()

    def wait_l(slot):
        pltpu.make_async_copy(l_hbm.at[:, :, pl.ds(0, LEFT * AL)], lb.at[slot], l_sem.at[slot]).wait()

    def psi_copy(k, st):
        own = gb.at[:, pl.ds(pl.multiple_of(zi * B, B), B), pl.ds(st * AL, AL)] if k == 0 else vv.at[0, :, :, pl.ds(st * AL, AL)]
        return pltpu.make_async_copy(psi_hbm.at[:, st], own, p_sem.at[k, st])

    for k in range(2):
        for st in range(PH):
            psi_copy(k, st).start()

    barrier = pltpu.get_barrier_semaphore()
    for q in range(1, LEFT):
        pl.semaphore_signal(barrier, inc=1, device_id=(zi, owner[q]), device_id_type=MESH)
    for k in range(1, Z):
        pl.semaphore_signal(barrier, inc=1, device_id=((zi + k) % Z, li), device_id_type=MESH)
    pl.semaphore_wait(barrier, LEFT + Z - 2)

    def rt_rows(left):
        return left // (LEFT // Q), pl.ds(pl.multiple_of((left % (LEFT // Q)) * SUB, SUB), SUB)

    my_q, my_rows = rt_rows(li)

    def r_first(k):
        dest = (zi + k) % Z
        return pltpu.make_async_remote_copy(
            src_ref=r_hbm.at[:, pl.ds(pl.multiple_of(dest * B + li * SUB, SUB), SUB), :],
            dst_ref=rt.at[my_q, :, my_rows, pl.ds(pl.multiple_of(zi * B, B), B)],
            send_sem=r1_send.at[k - 1], recv_sem=r1_recv.at[k - 1], device_id=(dest, li), device_id_type=MESH)

    def r_second(q):
        ref = rt.at[my_q, :, my_rows, :]
        return pltpu.make_async_remote_copy(
            src_ref=ref, dst_ref=ref, send_sem=r2_send.at[q - 1], recv_sem=r2_recv.at[q - 1],
            device_id=(zi, owner[q]), device_id_type=MESH)

    def r_second_landed(q):
        peer_q, peer_rows = rt_rows(owner[q])
        ref = rt.at[peer_q, :, peer_rows, :]
        return pltpu.make_async_remote_copy(
            src_ref=ref, dst_ref=ref, send_sem=r2_send.at[q - 1], recv_sem=r2_recv.at[q - 1],
            device_id=(zi, owner[q]), device_id_type=MESH)

    for k in range(1, Z):
        r_first(k).start()
    r_mine = pltpu.make_async_copy(
        r_hbm.at[:, pl.ds(pl.multiple_of(zi * B + li * SUB, SUB), SUB), :],
        rt.at[my_q, :, my_rows, pl.ds(pl.multiple_of(zi * B, B), B)], r_own)
    r_mine.start()
    load_l(0, 0)

    def ar_plane(idx, q):
        ref = ar_p.at[idx, li]
        return pltpu.make_async_remote_copy(
            src_ref=ref, dst_ref=ref, send_sem=ar_send.at[idx, q - 1], recv_sem=ar_recv.at[idx, q - 1],
            device_id=(zi, owner[q]), device_id_type=MESH)

    def ar_line(idx, k):
        ref = ar_z.at[idx, zi]
        return pltpu.make_async_remote_copy(
            src_ref=ref, dst_ref=ref, send_sem=ar_send.at[idx, LEFT - 2 + k], recv_sem=ar_recv.at[idx, LEFT - 2 + k],
            device_id=((zi + k) % Z, li), device_id_type=MESH)

    def ar_start(idx):
        ar_p[idx, li] = acc[...]
        for q in range(1, LEFT):
            ar_plane(idx, q).start()

    def ar_middle(idx):
        for q in range(1, LEFT):
            ar_plane(idx, q).wait()
        tot = ar_p[idx, 0]
        for q in range(1, LEFT):
            tot = tot + ar_p[idx, q]
        ar_z[idx, zi] = tot
        for k in range(1, Z):
            ar_line(idx, k).start()

    def ar_finish(idx):
        for k in range(1, Z):
            ar_line(idx, k).wait()
        return jnp.full((1, AL), jnp.sum((ar_z[idx, 0] + ar_z[idx, 1]) + (ar_z[idx, 2] + ar_z[idx, 3])), F32)

    def gb_piece(src_z, i):
        return gb.at[i // PH, pl.ds(pl.multiple_of(src_z * B, B), B), pl.ds(pl.multiple_of((i % PH) * AL, AL), AL)]

    def z_copy(up, hop, i):
        src_z = zi - (hop - 1) if up else zi + (hop - 1)
        return pltpu.make_async_remote_copy(
            src_ref=gb_piece(src_z, i), dst_ref=gb_piece(src_z, i),
            send_sem=z_send.at[0 if up else 1, hop - 1, i], recv_sem=z_recv.at[0 if up else 1, hop - 1, i],
            device_id=(zi + 1 if up else zi - 1, li), device_id_type=MESH)

    def z_sends(hop, up):
        return (zi < Z - 1) & (zi >= hop - 1) if up else (zi > 0) & (zi + hop - 1 <= Z - 1)

    def z_start(i):
        for up in (True, False):
            @pl.when(zi < Z - 1 if up else zi > 0)
            def _(up=up):
                z_copy(up, 1, i).start()

    def z_landed(up, hop, i):
        ref = gb_piece(zi - hop if up else zi + hop, i)
        return pltpu.make_async_remote_copy(
            src_ref=ref, dst_ref=ref,
            send_sem=z_send.at[0 if up else 1, hop - 1, i], recv_sem=z_recv.at[0 if up else 1, hop - 1, i],
            device_id=(zi - 1 if up else zi + 1, li), device_id_type=MESH)

    def stage_h(hop, i):
        for up in (True, False):
            @pl.when(z_sends(hop + 1, up))
            def _(up=up):
                z_landed(up, hop, i).wait_recv()
                z_copy(up, hop + 1, i).start()

    def stage_end(i):
        for up in (True, False):
            @pl.when(zi == Z - 1 if up else zi == 0)
            def _(up=up):
                for hop in (1, 2, 3):
                    z_landed(up, hop, i).wait_recv()

    def compute(i, part):
        c, u = i // PH, i % PH
        first = (1 - part) * 4
        tot = None
        for l in range(W):
            term = jnp.dot(
                xs[l, u].reshape(B, A), lb[c % 2, l, :, first * AL : (first + 4) * AL], precision=PREC, preferred_element_type=F32
            )
            tot = term if tot is None else tot + term
        for q in range(4):
            pb[i % 2, first + q] = tot[:, q * AL : (q + 1) * AL]

    def a_copy(i):
        return pltpu.make_async_remote_copy(
            src_ref=pb.at[i % 2, pl.ds(4, 4)], dst_ref=ra.at[i % 2], send_sem=a_send.at[i % 2], recv_sem=a_recv.at[i % 2],
            device_id=(zi, owner[4]), device_id_type=MESH)

    def b_copy(i, k):
        return pltpu.make_async_remote_copy(
            src_ref=sb.at[i % 2, k + 1], dst_ref=rb.at[i % 2, k], send_sem=b_send.at[i % 2, k], recv_sem=b_recv.at[i % 2, k],
            device_id=(zi, owner[k + 1]), device_id_type=MESH)

    def stage_b(i):
        a_copy(i).wait()
        for q in range(4):
            sb[i % 2, q] = pb[i % 2, q] + ra[i % 2, q]

    def stage_b_send(i):
        for k in (2, 0, 1):
            b_copy(i, k).start()

    def stage_c(s, i):
        for k in range(3):
            b_copy(i, k).wait()
        c, u = i // PH, i % PH
        val = (sb[i % 2, 0] + rb[i % 2, 2]) + (rb[i % 2, 0] + rb[i % 2, 1])
        gb[c, pl.ds(pl.multiple_of(zi * B, B), B), pl.ds(pl.multiple_of(u * AL, AL), AL)] = val
        acc[...] += rows8(val * vv[(s + 1) % 2, c, :, pl.ds(pl.multiple_of(u * AL, AL), AL)])

    def right_dot(t, slot):
        us[slot] = jnp.dot(rt[t % Q].reshape(W * D, Z * B), gb[t // Q], precision=PREC, preferred_element_type=F32)

    def mix(t, slot):
        c, dq = t // Q, t % Q
        beta_prev = cf[1:2, :]
        mat = jnp.concatenate(
            [jnp.concatenate([us[slot, pl.ds(r * D + g * 8, 8), pl.ds(st * AL, AL)] for r in range(W) for st in range(PH)], axis=0)
             for g in range(D // 8)], axis=1)
        res = jnp.dot(wb[...], mat, precision=PREC, preferred_element_type=F32)
        for g in range(D // 8):
            for l in range(W):
                for uv in range(PH):
                    old = xb[slot, l, uv, pl.ds(g * 8, 8), :]
                    row = pl.multiple_of((uv % 2) * B + dq * D + g * 8, 8)
                    lane = pl.multiple_of((uv // 2) * A + c * AL, AL)
                    j = (l * PH + uv) * 8
                    lb[1, l, pl.ds(row, 8), pl.ds(lane, AL)] = res[j : j + 8, g * AL : (g + 1) * AL] - beta_prev * old

    def old_copy(s, t, slot):
        return pltpu.make_async_copy(
            hist_hbm.at[s % 2, :, :, t % Q, :, pl.ds(pl.multiple_of((t // Q) * AL, AL), AL)], xb.at[slot], x_sem.at[slot])

    def hist_copy(s):
        return pltpu.make_async_copy(xs, hist_hbm.at[(s + 1) % 2], h_sem)

    def clear():
        def quarter(i, _):
            for l in range(W):
                for h in range(4):
                    xs[l, h, i] = jnp.zeros((D, A), F32)
            return 0

        lax.fori_loop(0, Q, quarter, 0)
        us[...] = jnp.zeros_like(us)
        xb[...] = jnp.zeros_like(xb)
        vv[1] = jnp.zeros((C, B, PH * AL), F32)
        cf[...] = jnp.zeros_like(cf)
        for st in range(PH):
            psi_copy(1, st).wait()

    for st in range(PH):
        psi_copy(0, st).wait()

    def vv_piece(k, i):
        return vv.at[k, i // PH, :, pl.ds(pl.multiple_of((i % PH) * AL, AL), AL)]

    def gather_step(i):
        @pl.when(i < S)
        def _():
            z_start(i)

        @pl.when((i >= 2) & (i < S + 2))
        def _():
            stage_h(1, i - 2)

        @pl.when((i >= 4) & (i < S + 4))
        def _():
            stage_h(2, i - 4)

    LEAD = 10

    def norm():
        acc[...] = jnp.zeros_like(acc)

        def piece(i, _):
            val = vv_piece(0, i)[...]
            acc[...] += rows8(val * val)
            return 0

        lax.fori_loop(0, S, piece, 0)
        ar_start(0)

    def to_unit():
        scale = jnp.sqrt(COUNT / ar_finish(0))
        cf[2:3, :] = scale

        def piece(i, _):
            ref = vv_piece(0, i)
            ref[...] = ref[...] * scale
            return 0

        lax.fori_loop(0, S, piece, 0)

    def spread_r():
        r_mine.wait()
        for k in range(1, Z):
            r_first(k).wait()
        for q in range(1, LEFT):
            r_second(q).start()

    def gather(i, _):
        gather_step(i)
        for when, fn in ((0, clear), (1, norm), (2, lambda: ar_middle(0)), (3, spread_r), (5, to_unit)):
            pl.when(i == when)(fn)
        return 0

    lax.fori_loop(0, LEAD, gather, 0)
    for q in range(1, LEFT):
        r_second(q).wait_send()
        r_second_landed(q).wait_recv()

    def step(s, _):
        @pl.when(s > 0)
        def _():
            acc[...] = jnp.zeros_like(acc)

            def boundary(i):
                stage_b(i)

                @pl.when(i >= 1)
                def _():
                    stage_c(s, i - 1)

                stage_b_send(i)

                @pl.when(s < STEPS)
                def _():
                    @pl.when(i == 1)
                    def _():
                        @pl.when(zi < Z - 1)
                        def _():
                            pl.semaphore_wait(ready.at[0], 1)

                        @pl.when(zi > 0)
                        def _():
                            pl.semaphore_wait(ready.at[1], 1)

                    @pl.when(i >= 3)
                    def _():
                        stage_h(2, i - 3)

                    @pl.when(i >= 2)
                    def _():
                        stage_h(1, i - 2)

                    @pl.when(i >= 1)
                    def _():
                        z_start(i - 1)

            wait_l(0)
            load_l(1, 1)
            compute(0, 0)
            a_copy(0).start()

            def pair(i, _):
                c = i // PH

                @pl.when(i % PH == PH - 1)
                def _():
                    wait_l((c + 1) % 2)

                compute(i, 1)
                compute(i + 1, 0)

                @pl.when((i % PH == PH - 1) & ((c < C - 2) | (s < STEPS)))
                def _():
                    load_l((c + 2) % C, c % 2)

                boundary(i)
                a_copy(i + 1).start()
                return 0

            lax.fori_loop(0, S - 1, pair, 0)
            compute(S - 1, 1)
            boundary(S - 1)

        @pl.when((s > 0) & (s < STEPS))
        def _():
            hist_copy(s).start()

        def right_step(t, _):
            slot = t % 2

            @pl.when(s < STEPS)
            def _():
                @pl.when(t % Q == 0)
                def _():
                    for k in range(4):
                        stage_end((t // Q) * PH + k)

                @pl.when(s > 1)
                def _():
                    old_copy(s, t, slot).start()

                    @pl.when(t > 0)
                    def _():
                        old_copy(s, t - 1, 1 - slot).wait()

                mix(jnp.maximum(t - 1, 0), 1 - slot)
                right_dot(t, slot)

            @pl.when(s == 0)
            def _():
                for k in range(PH // Q):
                    gather_step(t * (PH // Q) + k + LEAD)

            @pl.when(s > 0)
            def _():
                idx = s * 2 - 1

                def at(when, fn, hop=False):
                    @pl.when((t == when) & (s < STEPS) if hop else t == when)
                    def _():
                        fn()

                at(0, lambda: (stage_h(2, S - 3), stage_h(1, S - 2)), True)
                at(1, lambda: (stage_c(s, S - 1), ar_start(idx)))
                at(1, lambda: z_start(S - 1), True)
                at(1, lambda: stage_h(2, S - 2), True)
                at(2, lambda: ar_middle(idx))
                at(2, lambda: stage_h(1, S - 1), True)

                def ortho():
                    alpha = ar_finish(idx) / COUNT
                    beta_prev = cf[1:2, :]
                    cf[0:1, :] = alpha
                    acc[...] = jnp.zeros_like(acc)

                    def piece(i, _):
                        val = gb_piece(zi, i)[...] - alpha * vv_piece((s + 1) % 2, i)[...] - beta_prev * vv_piece(s % 2, i)[...]
                        vv_piece(s % 2, i)[...] = val
                        acc[...] += rows8(val * val)
                        return 0

                    lax.fori_loop(0, S, piece, 0)
                    ar_start(idx + 1)

                at(3, lambda: stage_h(2, S - 1), True)
                at(3, ortho)
                at(4, lambda: ar_middle(idx + 1))

                def norm_out():
                    beta = jnp.sqrt(ar_finish(idx + 1) / COUNT)
                    inv = 1.0 / beta
                    cf[2:3, :] = inv
                    cf[3:4, :] = beta
                    coef_ref[s - 1, 0:1, :] = cf[0:1, :]
                    coef_ref[s - 1, 1:2, :] = beta

                    def piece(i, _):
                        ref = vv_piece(s % 2, i)
                        ref[...] = ref[...] * inv
                        return 0

                    lax.fori_loop(0, S, piece, 0)

                at(5, norm_out)

            return 0

        lax.fori_loop(0, RT, right_step, 0)

        @pl.when(s < STEPS)
        def _():
            @pl.when(s > 1)
            def _():
                old_copy(s, RT - 1, (RT - 1) % 2).wait()

            mix(RT - 1, (RT - 1) % 2)

            @pl.when(s > 0)
            def _():
                hist_copy(s).wait()

            alpha, inv = cf[0:1, 0:1], cf[2:3, 0:1]

            def combine(k, _):
                l, uv = k // PH, k % PH
                for dq in range(Q):
                    new = lb[1, l, pl.ds(pl.multiple_of((uv % 2) * B + dq * D, D), D), pl.ds(pl.multiple_of((uv // 2) * A, A), A)]
                    xs[l, uv, dq] = (new - alpha * xs[l, uv, dq]) * inv
                return 0

            lax.fori_loop(0, W * PH, combine, 0)

            def sent(i, _):
                for hop in (1, 2, 3):
                    for up in (True, False):
                        @pl.when(z_sends(hop, up))
                        def _(up=up, hop=hop):
                            z_copy(up, hop, i).wait_send()
                return 0

            lax.fori_loop(0, S, sent, 0)

            @pl.when((zi > 0) & (s < STEPS - 1))
            def _():
                pl.semaphore_signal(ready.at[0], inc=1, device_id=(zi - 1, li), device_id_type=MESH)

            @pl.when((zi < Z - 1) & (s < STEPS - 1))
            def _():
                pl.semaphore_signal(ready.at[1], inc=1, device_id=(zi + 1, li), device_id_type=MESH)

            cf[1:2, :] = cf[3:4, :]

        return 0

    lax.fori_loop(0, STEPS + 1, step, 0)

    out_copies = [
        pltpu.make_async_copy(vv.at[STEPS % 2, :, :, pl.ds(st * AL, AL)], out_hbm.at[:, st], o_sem.at[st]) for st in range(PH)
    ]
    for copy in out_copies:
        copy.start()
    for copy in out_copies:
        copy.wait()


def lanczos_kernel(psi, l_env, r_env, mix):
    hbm = pl.BlockSpec(memory_space=pltpu.HBM)
    vmem = pl.BlockSpec(memory_space=pltpu.VMEM)
    dma = pltpu.SemaphoreType.DMA
    piece = (B, AL)
    n_ar = 2 * STEPS + 1
    return pl.pallas_call(
        kernel,
        in_specs=[hbm, hbm, hbm, vmem],
        out_specs=[hbm, vmem, hbm],
        out_shape=[
            jax.ShapeDtypeStruct((C, PH) + piece, F32),
            jax.ShapeDtypeStruct((STEPS, 8, AL), F32),
            jax.ShapeDtypeStruct((2, W, PH, Q, D, A), F32),
        ],
        scratch_shapes=[
            pltpu.VMEM((W, PH, Q, D, A), F32),
            pltpu.VMEM((2, W, A, LEFT * AL), F32),
            pltpu.VMEM((2, 8) + piece, F32),
            pltpu.VMEM((2, 4) + piece, F32),
            pltpu.VMEM((2, 4) + piece, F32),
            pltpu.VMEM((2, 3) + piece, F32),
            pltpu.VMEM((C, Z * B, PH * AL), F32),
            pltpu.VMEM((2, C, B, PH * AL), F32),
            pltpu.VMEM((Q, W, D, Z * B), F32),
            pltpu.VMEM((2, W * D, PH * AL), F32),
            pltpu.VMEM((2, W, PH, D, AL), F32),
            pltpu.VMEM((8, AL), F32),
            pltpu.VMEM((8, AL), F32),
            pltpu.VMEM((n_ar, LEFT, 8, AL), F32),
            pltpu.VMEM((n_ar, Z, 8, AL), F32),
            dma((2, PH)), dma((2,)), dma, dma((2,)), dma((PH,)), dma((3,)), dma((3,)), dma((7,)), dma((7,)), dma,
            dma((2,)), dma((2,)), dma((2, 3)), dma((2, 3)), dma((2, 3, S)), dma((2, 3, S)),
            dma((n_ar, LEFT + Z - 2)), dma((n_ar, LEFT + Z - 2)), pltpu.SemaphoreType.REGULAR((2,)),
        ],
        compiler_params=pltpu.CompilerParams(
            vmem_limit_bytes=67_043_328, collective_id=1, has_side_effects=True),
        name="lanczos",
    )(psi, l_env, r_env, mix)


def solution(mesh):
    def lanczos(psi, left_env, right_env, mpo):
        own = psi.reshape(C, AL, PH, B).transpose(0, 2, 3, 1)
        l_env = left_env.transpose(1, 0, 2)
        r_env = right_env.transpose(1, 2, 0)
        mix = mpo.reshape(W, W, PH, PH).transpose(0, 3, 1, 2).reshape(W * PH, W * PH)
        mix = jnp.kron(mix, jnp.eye(8, dtype=F32))
        out, coef, _ = lanczos_kernel(own, l_env, r_env, mix)
        vec = out.transpose(0, 3, 1, 2).reshape(psi.shape)
        return coef[:, 0, 0], coef[:, 1, 0], vec

    return jax.shard_map(
        lanczos,
        mesh=mesh,
        in_specs=(P("left", None, None, "right"), P("left", None, None), P("right", None, None), P()),
        out_specs=(P(), P(), P("left", None, None, "right")),
        check_vma=False,
    )
```

```python
import jax
import jax.numpy as jnp
from jax import lax
from jax.experimental import pallas as pl
from jax.experimental.pallas import tpu as pltpu
from jax.sharding import PartitionSpec as P

STEPS = 4
PREC = lax.Precision.HIGHEST
MESH = pl.DeviceIdType.MESH
F32 = jnp.float32

Z = 4
LEFT = 8
A = 512
B = 256
PH = 4
W = 5
C = 4
AL = A // C
S = C * PH
Q = 2
D = B // Q
SUB = B // LEFT
AHEAD = 3
RT = C * Q
COUNT = float(LEFT * Z * S * B * AL)


def place(left):
    return left // 4, (left // 2) % 2, left % 2


def left_of(y, x, core):
    return (y * 2 + x) * 2 + core


def rows8(value):
    return jnp.sum(value.reshape(-1, 8, AL), axis=0)


def kernel(psi_hbm, l_hbm, r_hbm, wb, out_hbm, coef_ref, hist_hbm,
           xs, lb, pb, ra, sb, rb, gb, vv, rt, us, xb, cf, acc, ar_p, ar_z,
           p_sem, l_sem, h_sem, x_sem, o_sem, r1_send, r1_recv, r2_send, r2_recv, r_own,
           a_send, a_recv, b_send, b_recv, z_send, z_recv, ar_send, ar_recv, ready):
    zi = lax.axis_index("right")
    li = lax.axis_index("left")
    y, x, core = place(li)
    owner = [left_of(y, x, core), left_of(y, 1 - x, core), left_of(1 - y, x, core), left_of(1 - y, 1 - x, core),
             left_of(y, x, 1 - core), left_of(y, 1 - x, 1 - core), left_of(1 - y, x, 1 - core), left_of(1 - y, 1 - x, 1 - core)]

    def load_l(c, slot):
        for q in range(LEFT):
            pltpu.make_async_copy(
                l_hbm.at[:, :, pl.ds(pl.multiple_of(owner[q] * A + c * AL, AL), AL)],
                lb.at[slot, :, :, pl.ds(q * AL, AL)],
                l_sem.at[slot],
            ).start()

    def wait_l(slot):
        pltpu.make_async_copy(l_hbm.at[:, :, pl.ds(0, LEFT * AL)], lb.at[slot], l_sem.at[slot]).wait()

    def psi_copy(k, st):
        own = gb.at[:, pl.ds(pl.multiple_of(zi * B, B), B), pl.ds(st * AL, AL)] if k == 0 else vv.at[0, :, :, pl.ds(st * AL, AL)]
        return pltpu.make_async_copy(psi_hbm.at[:, st], own, p_sem.at[k, st])

    for k in range(2):
        for st in range(PH):
            psi_copy(k, st).start()

    barrier = pltpu.get_barrier_semaphore()
    for q in range(1, LEFT):
        pl.semaphore_signal(barrier, inc=1, device_id=(zi, owner[q]), device_id_type=MESH)
    for k in range(1, Z):
        pl.semaphore_signal(barrier, inc=1, device_id=((zi + k) % Z, li), device_id_type=MESH)
    pl.semaphore_wait(barrier, LEFT + Z - 2)

    def rt_rows(left):
        return left // (LEFT // Q), pl.ds(pl.multiple_of((left % (LEFT // Q)) * SUB, SUB), SUB)

    my_q, my_rows = rt_rows(li)

    def r_first(k):
        dest = (zi + k) % Z
        return pltpu.make_async_remote_copy(
            src_ref=r_hbm.at[:, pl.ds(pl.multiple_of(dest * B + li * SUB, SUB), SUB), :],
            dst_ref=rt.at[my_q, :, my_rows, pl.ds(pl.multiple_of(zi * B, B), B)],
            send_sem=r1_send.at[k - 1], recv_sem=r1_recv.at[k - 1], device_id=(dest, li), device_id_type=MESH)

    def r_second(q):
        ref = rt.at[my_q, :, my_rows, :]
        return pltpu.make_async_remote_copy(
            src_ref=ref, dst_ref=ref, send_sem=r2_send.at[q - 1], recv_sem=r2_recv.at[q - 1],
            device_id=(zi, owner[q]), device_id_type=MESH)

    def r_second_landed(q):
        peer_q, peer_rows = rt_rows(owner[q])
        ref = rt.at[peer_q, :, peer_rows, :]
        return pltpu.make_async_remote_copy(
            src_ref=ref, dst_ref=ref, send_sem=r2_send.at[q - 1], recv_sem=r2_recv.at[q - 1],
            device_id=(zi, owner[q]), device_id_type=MESH)

    for k in range(1, Z):
        r_first(k).start()
    r_mine = pltpu.make_async_copy(
        r_hbm.at[:, pl.ds(pl.multiple_of(zi * B + li * SUB, SUB), SUB), :],
        rt.at[my_q, :, my_rows, pl.ds(pl.multiple_of(zi * B, B), B)], r_own)
    r_mine.start()
    load_l(0, 0)

    def ar_plane(idx, q):
        ref = ar_p.at[idx, li]
        return pltpu.make_async_remote_copy(
            src_ref=ref, dst_ref=ref, send_sem=ar_send.at[idx, q - 1], recv_sem=ar_recv.at[idx, q - 1],
            device_id=(zi, owner[q]), device_id_type=MESH)

    def ar_line(idx, k):
        ref = ar_z.at[idx, zi]
        return pltpu.make_async_remote_copy(
            src_ref=ref, dst_ref=ref, send_sem=ar_send.at[idx, LEFT - 2 + k], recv_sem=ar_recv.at[idx, LEFT - 2 + k],
            device_id=((zi + k) % Z, li), device_id_type=MESH)

    def ar_start(idx):
        ar_p[idx, li] = acc[...]
        for q in range(1, LEFT):
            ar_plane(idx, q).start()

    def ar_middle(idx):
        for q in range(1, LEFT):
            ar_plane(idx, q).wait()
        tot = ar_p[idx, 0]
        for q in range(1, LEFT):
            tot = tot + ar_p[idx, q]
        ar_z[idx, zi] = tot
        for k in range(1, Z):
            ar_line(idx, k).start()

    def ar_finish(idx):
        for k in range(1, Z):
            ar_line(idx, k).wait()
        return jnp.full((1, AL), jnp.sum((ar_z[idx, 0] + ar_z[idx, 1]) + (ar_z[idx, 2] + ar_z[idx, 3])), F32)

    def gb_piece(src_z, i):
        return gb.at[i // PH, pl.ds(pl.multiple_of(src_z * B, B), B), pl.ds(pl.multiple_of((i % PH) * AL, AL), AL)]

    def z_copy(up, hop, i):
        src_z = zi - (hop - 1) if up else zi + (hop - 1)
        return pltpu.make_async_remote_copy(
            src_ref=gb_piece(src_z, i), dst_ref=gb_piece(src_z, i),
            send_sem=z_send.at[0 if up else 1, hop - 1, i], recv_sem=z_recv.at[0 if up else 1, hop - 1, i],
            device_id=(zi + 1 if up else zi - 1, li), device_id_type=MESH)

    def z_sends(hop, up):
        return (zi < Z - 1) & (zi >= hop - 1) if up else (zi > 0) & (zi + hop - 1 <= Z - 1)

    def z_start(i):
        for up in (True, False):
            @pl.when(zi < Z - 1 if up else zi > 0)
            def _(up=up):
                z_copy(up, 1, i).start()

    def z_landed(up, hop, i):
        ref = gb_piece(zi - hop if up else zi + hop, i)
        return pltpu.make_async_remote_copy(
            src_ref=ref, dst_ref=ref,
            send_sem=z_send.at[0 if up else 1, hop - 1, i], recv_sem=z_recv.at[0 if up else 1, hop - 1, i],
            device_id=(zi - 1 if up else zi + 1, li), device_id_type=MESH)

    def stage_h(hop, i):
        for up in (True, False):
            @pl.when(z_sends(hop + 1, up))
            def _(up=up):
                z_landed(up, hop, i).wait_recv()
                z_copy(up, hop + 1, i).start()

    def stage_end(i):
        for up in (True, False):
            @pl.when(zi == Z - 1 if up else zi == 0)
            def _(up=up):
                for hop in (1, 2, 3):
                    z_landed(up, hop, i).wait_recv()

    def compute(i, part):
        c, u = i // PH, i % PH
        first = (1 - part) * 4
        tot = None
        for l in range(W):
            term = jnp.dot(
                xs[l, u].reshape(B, A), lb[c % 2, l, :, first * AL : (first + 4) * AL], precision=PREC, preferred_element_type=F32
            )
            tot = term if tot is None else tot + term
        for q in range(4):
            pb[i % 2, first + q] = tot[:, q * AL : (q + 1) * AL]

    def a_copy(i):
        return pltpu.make_async_remote_copy(
            src_ref=pb.at[i % 2, pl.ds(4, 4)], dst_ref=ra.at[i % 2], send_sem=a_send.at[i % 2], recv_sem=a_recv.at[i % 2],
            device_id=(zi, owner[4]), device_id_type=MESH)

    def b_copy(i, k):
        return pltpu.make_async_remote_copy(
            src_ref=sb.at[i % 2, k + 1], dst_ref=rb.at[i % 2, k], send_sem=b_send.at[i % 2, k], recv_sem=b_recv.at[i % 2, k],
            device_id=(zi, owner[k + 1]), device_id_type=MESH)

    def stage_b(i):
        a_copy(i).wait()
        for q in range(4):
            sb[i % 2, q] = pb[i % 2, q] + ra[i % 2, q]

    def stage_b_send(i):
        for k in (2, 0, 1):
            b_copy(i, k).start()

    def stage_c(s, i):
        for k in range(3):
            b_copy(i, k).wait()
        c, u = i // PH, i % PH
        val = (sb[i % 2, 0] + rb[i % 2, 2]) + (rb[i % 2, 0] + rb[i % 2, 1])
        gb[c, pl.ds(pl.multiple_of(zi * B, B), B), pl.ds(pl.multiple_of(u * AL, AL), AL)] = val
        acc[...] += rows8(val * vv[(s + 1) % 2, c, :, pl.ds(pl.multiple_of(u * AL, AL), AL)])

    def right_dot(t, slot):
        us[slot] = jnp.dot(rt[t % Q].reshape(W * D, Z * B), gb[t // Q], precision=PREC, preferred_element_type=F32)

    def mix(t, slot):
        c, dq = t // Q, t % Q
        beta_prev = cf[1:2, :]
        mat = jnp.concatenate(
            [jnp.concatenate([us[slot, pl.ds(r * D + g * 8, 8), pl.ds(st * AL, AL)] for r in range(W) for st in range(PH)], axis=0)
             for g in range(D // 8)], axis=1)
        res = jnp.dot(wb[...], mat, precision=PREC, preferred_element_type=F32)
        for g in range(D // 8):
            for l in range(W):
                for uv in range(PH):
                    old = xb[slot, l, uv, pl.ds(g * 8, 8), :]
                    row = pl.multiple_of((uv % 2) * B + dq * D + g * 8, 8)
                    lane = pl.multiple_of((uv // 2) * A + c * AL, AL)
                    j = (l * PH + uv) * 8
                    lb[1, l, pl.ds(row, 8), pl.ds(lane, AL)] = res[j : j + 8, g * AL : (g + 1) * AL] - beta_prev * old

    def old_copy(s, t, slot):
        return pltpu.make_async_copy(
            hist_hbm.at[s % 2, :, :, t % Q, :, pl.ds(pl.multiple_of((t // Q) * AL, AL), AL)], xb.at[slot], x_sem.at[slot])

    def hist_copy(s):
        return pltpu.make_async_copy(xs, hist_hbm.at[(s + 1) % 2], h_sem)

    def clear():
        def quarter(i, _):
            for l in range(W):
                for h in range(4):
                    xs[l, h, i] = jnp.zeros((D, A), F32)
            return 0

        lax.fori_loop(0, Q, quarter, 0)
        us[...] = jnp.zeros_like(us)
        xb[...] = jnp.zeros_like(xb)
        vv[1] = jnp.zeros((C, B, PH * AL), F32)
        cf[...] = jnp.zeros_like(cf)
        for st in range(PH):
            psi_copy(1, st).wait()

    for st in range(PH):
        psi_copy(0, st).wait()

    def vv_piece(k, i):
        return vv.at[k, i // PH, :, pl.ds(pl.multiple_of((i % PH) * AL, AL), AL)]

    def gather_step(i):
        @pl.when(i < S - AHEAD)
        def _():
            z_start(i + AHEAD)

        @pl.when((i >= 2) & (i < S + 2))
        def _():
            stage_h(1, i - 2)

        @pl.when((i >= 4) & (i < S + 4))
        def _():
            stage_h(2, i - 4)

    LEAD = 10
    for i in range(AHEAD):
        z_start(i)

    def norm():
        acc[...] = jnp.zeros_like(acc)

        def piece(i, _):
            val = vv_piece(0, i)[...]
            acc[...] += rows8(val * val)
            return 0

        lax.fori_loop(0, S, piece, 0)
        ar_start(0)

    def to_unit():
        scale = jnp.sqrt(COUNT / ar_finish(0))
        cf[2:3, :] = scale

        def piece(i, _):
            ref = vv_piece(0, i)
            ref[...] = ref[...] * scale
            return 0

        lax.fori_loop(0, S, piece, 0)

    def spread_r():
        r_mine.wait()
        for k in range(1, Z):
            r_first(k).wait()
        for q in range(1, LEFT):
            r_second(q).start()

    def gather(i, _):
        gather_step(i)
        for when, fn in ((0, clear), (1, norm), (2, lambda: ar_middle(0)), (3, spread_r), (5, to_unit)):
            pl.when(i == when)(fn)
        return 0

    lax.fori_loop(0, LEAD, gather, 0)
    for q in range(1, LEFT):
        r_second(q).wait_send()
        r_second_landed(q).wait_recv()

    def step(s, _):
        @pl.when(s > 0)
        def _():
            acc[...] = jnp.zeros_like(acc)

            def boundary(i):
                stage_b(i)

                @pl.when(i >= 1)
                def _():
                    stage_c(s, i - 1)

                stage_b_send(i)

                @pl.when(s < STEPS)
                def _():
                    @pl.when(i == 1)
                    def _():
                        @pl.when(zi < Z - 1)
                        def _():
                            pl.semaphore_wait(ready.at[0], 1)

                        @pl.when(zi > 0)
                        def _():
                            pl.semaphore_wait(ready.at[1], 1)

                    @pl.when(i >= 3)
                    def _():
                        stage_h(2, i - 3)

                    @pl.when(i >= 2)
                    def _():
                        stage_h(1, i - 2)

                    @pl.when(i >= 1)
                    def _():
                        z_start(i - 1)

            wait_l(0)
            load_l(1, 1)
            compute(0, 0)
            a_copy(0).start()

            def pair(i, _):
                c = i // PH

                @pl.when(i % PH == PH - 1)
                def _():
                    wait_l((c + 1) % 2)

                compute(i, 1)
                compute(i + 1, 0)

                @pl.when((i % PH == PH - 1) & ((c < C - 2) | (s < STEPS)))
                def _():
                    load_l((c + 2) % C, c % 2)

                boundary(i)
                a_copy(i + 1).start()
                return 0

            lax.fori_loop(0, S - 1, pair, 0)
            compute(S - 1, 1)
            boundary(S - 1)

        @pl.when((s > 0) & (s < STEPS))
        def _():
            hist_copy(s).start()

        def right_step(t, _):
            slot = t % 2

            @pl.when(s < STEPS)
            def _():
                @pl.when(t % Q == 0)
                def _():
                    for k in range(4):
                        stage_end((t // Q) * PH + k)

                @pl.when(s > 1)
                def _():
                    old_copy(s, t, slot).start()

                    @pl.when(t > 0)
                    def _():
                        old_copy(s, t - 1, 1 - slot).wait()

                mix(jnp.maximum(t - 1, 0), 1 - slot)
                right_dot(t, slot)

            @pl.when(s == 0)
            def _():
                for k in range(PH // Q):
                    gather_step(t * (PH // Q) + k + LEAD)

            @pl.when(s > 0)
            def _():
                idx = s * 2 - 1

                def at(when, fn, hop=False):
                    @pl.when((t == when) & (s < STEPS) if hop else t == when)
                    def _():
                        fn()

                at(0, lambda: (stage_h(2, S - 3), stage_h(1, S - 2)), True)
                at(1, lambda: (stage_c(s, S - 1), ar_start(idx)))
                at(1, lambda: z_start(S - 1), True)
                at(1, lambda: stage_h(2, S - 2), True)
                at(2, lambda: ar_middle(idx))
                at(2, lambda: stage_h(1, S - 1), True)

                def ortho():
                    alpha = ar_finish(idx) / COUNT
                    beta_prev = cf[1:2, :]
                    cf[0:1, :] = alpha
                    acc[...] = jnp.zeros_like(acc)

                    def piece(i, _):
                        val = gb_piece(zi, i)[...] - alpha * vv_piece((s + 1) % 2, i)[...] - beta_prev * vv_piece(s % 2, i)[...]
                        vv_piece(s % 2, i)[...] = val
                        acc[...] += rows8(val * val)
                        return 0

                    lax.fori_loop(0, S, piece, 0)
                    ar_start(idx + 1)

                at(3, lambda: stage_h(2, S - 1), True)
                at(3, ortho)
                at(4, lambda: ar_middle(idx + 1))

                def norm_out():
                    beta = jnp.sqrt(ar_finish(idx + 1) / COUNT)
                    inv = 1.0 / beta
                    cf[2:3, :] = inv
                    cf[3:4, :] = beta
                    coef_ref[s - 1, 0:1, :] = cf[0:1, :]
                    coef_ref[s - 1, 1:2, :] = beta

                    def piece(i, _):
                        ref = vv_piece(s % 2, i)
                        ref[...] = ref[...] * inv
                        return 0

                    lax.fori_loop(0, S, piece, 0)

                at(5, norm_out)

            return 0

        lax.fori_loop(0, RT, right_step, 0)

        @pl.when(s < STEPS)
        def _():
            @pl.when(s > 1)
            def _():
                old_copy(s, RT - 1, (RT - 1) % 2).wait()

            mix(RT - 1, (RT - 1) % 2)

            @pl.when(s > 0)
            def _():
                hist_copy(s).wait()

            alpha, inv = cf[0:1, 0:1], cf[2:3, 0:1]

            def combine(k, _):
                l, uv = k // PH, k % PH
                for dq in range(Q):
                    new = lb[1, l, pl.ds(pl.multiple_of((uv % 2) * B + dq * D, D), D), pl.ds(pl.multiple_of((uv // 2) * A, A), A)]
                    xs[l, uv, dq] = (new - alpha * xs[l, uv, dq]) * inv
                return 0

            lax.fori_loop(0, W * PH, combine, 0)

            def sent(i, _):
                for hop in (1, 2, 3):
                    for up in (True, False):
                        @pl.when(z_sends(hop, up))
                        def _(up=up, hop=hop):
                            z_copy(up, hop, i).wait_send()
                return 0

            lax.fori_loop(0, S, sent, 0)

            @pl.when((zi > 0) & (s < STEPS - 1))
            def _():
                pl.semaphore_signal(ready.at[0], inc=1, device_id=(zi - 1, li), device_id_type=MESH)

            @pl.when((zi < Z - 1) & (s < STEPS - 1))
            def _():
                pl.semaphore_signal(ready.at[1], inc=1, device_id=(zi + 1, li), device_id_type=MESH)

            cf[1:2, :] = cf[3:4, :]

        return 0

    lax.fori_loop(0, STEPS + 1, step, 0)

    out_copies = [
        pltpu.make_async_copy(vv.at[STEPS % 2, :, :, pl.ds(st * AL, AL)], out_hbm.at[:, st], o_sem.at[st]) for st in range(PH)
    ]
    for copy in out_copies:
        copy.start()
    for copy in out_copies:
        copy.wait()


def lanczos_kernel(psi, l_env, r_env, mix):
    hbm = pl.BlockSpec(memory_space=pltpu.HBM)
    vmem = pl.BlockSpec(memory_space=pltpu.VMEM)
    dma = pltpu.SemaphoreType.DMA
    piece = (B, AL)
    n_ar = 2 * STEPS + 1
    return pl.pallas_call(
        kernel,
        in_specs=[hbm, hbm, hbm, vmem],
        out_specs=[hbm, vmem, hbm],
        out_shape=[
            jax.ShapeDtypeStruct((C, PH) + piece, F32),
            jax.ShapeDtypeStruct((STEPS, 8, AL), F32),
            jax.ShapeDtypeStruct((2, W, PH, Q, D, A), F32),
        ],
        scratch_shapes=[
            pltpu.VMEM((W, PH, Q, D, A), F32),
            pltpu.VMEM((2, W, A, LEFT * AL), F32),
            pltpu.VMEM((2, 8) + piece, F32),
            pltpu.VMEM((2, 4) + piece, F32),
            pltpu.VMEM((2, 4) + piece, F32),
            pltpu.VMEM((2, 3) + piece, F32),
            pltpu.VMEM((C, Z * B, PH * AL), F32),
            pltpu.VMEM((2, C, B, PH * AL), F32),
            pltpu.VMEM((Q, W, D, Z * B), F32),
            pltpu.VMEM((2, W * D, PH * AL), F32),
            pltpu.VMEM((2, W, PH, D, AL), F32),
            pltpu.VMEM((8, AL), F32),
            pltpu.VMEM((8, AL), F32),
            pltpu.VMEM((n_ar, LEFT, 8, AL), F32),
            pltpu.VMEM((n_ar, Z, 8, AL), F32),
            dma((2, PH)), dma((2,)), dma, dma((2,)), dma((PH,)), dma((3,)), dma((3,)), dma((7,)), dma((7,)), dma,
            dma((2,)), dma((2,)), dma((2, 3)), dma((2, 3)), dma((2, 3, S)), dma((2, 3, S)),
            dma((n_ar, LEFT + Z - 2)), dma((n_ar, LEFT + Z - 2)), pltpu.SemaphoreType.REGULAR((2,)),
        ],
        compiler_params=pltpu.CompilerParams(
            vmem_limit_bytes=67_043_328, collective_id=1, has_side_effects=True),
        name="lanczos",
    )(psi, l_env, r_env, mix)


def solution(mesh):
    def lanczos(psi, left_env, right_env, mpo):
        own = psi.reshape(C, AL, PH, B).transpose(0, 2, 3, 1)
        l_env = left_env.transpose(1, 0, 2)
        r_env = right_env.transpose(1, 2, 0)
        mix = mpo.reshape(W, W, PH, PH).transpose(0, 3, 1, 2).reshape(W * PH, W * PH)
        mix = jnp.kron(mix, jnp.eye(8, dtype=F32))
        out, coef, _ = lanczos_kernel(own, l_env, r_env, mix)
        vec = out.transpose(0, 3, 1, 2).reshape(psi.shape)
        return coef[:, 0, 0], coef[:, 1, 0], vec

    return jax.shard_map(
        lanczos,
        mesh=mesh,
        in_specs=(P("left", None, None, "right"), P("left", None, None), P("right", None, None), P()),
        out_specs=(P(), P(), P("left", None, None, "right")),
        check_vma=False,
    )
```
